32 devices in a mesh: dp: 4 (over x, y), tp: 8 (over z, core).
Axes of the slice: x: 2, y: 2, z: 4, core: 2. Of those that a mesh axis runs over, the one named last changes fastest.
Arguments:
- x: bfloat16 [8192, 6144], P(('dp', 'tp')), parts along dimension 0
- gain_a: bfloat16 [6144], replicated
- wq: bfloat16 [6144, 6144], P(None, 'tp')
- wk: bfloat16 [6144, 1024], P(None, 'tp')
- wv: bfloat16 [6144, 1024], P(None, 'tp')
- wo: bfloat16 [6144, 6144], P('tp')
- gain_m: bfloat16 [6144], replicated
- w_gate: bfloat16 [6144, 16384], P(None, 'tp')
- w_up: bfloat16 [6144, 16384], P(None, 'tp')
- w_down: bfloat16 [16384, 6144], P('tp')
Outputs:
- output: bfloat16 [8192, 6144], P(('dp', 'tp')), parts along dimension 0
There are 4 independent parts. The reference program is written for one: setup_inputs(seed, part) draws one part's arguments, and reference() takes and returns one part's arrays. A program takes and returns all parts, laid end to end along the dimension named above; an argument that names none is the same for every part.
All inputs are finite; a program needn't handle non-finite values.
Results may differ from the reference program's by a relative error of at most 0.017.
Values are sent between devices in bfloat16 or wider.
A program may use at most 2 GiB of HBM per device.

```python
import jax
import jax.numpy as jnp
from jax import lax

ROWS = 2048
D = 6144
HEADS = 48
KV_HEADS = 8
HEAD = 128
FF = 16384
THETA = 10000


def setup_inputs(seed: int = 0, part: int = 0) -> dict:
    kx, kn, kq, kk, kv, ko, km, kg, ku, kd = jax.random.split(jax.random.key(seed), 10)

    def weights(key, rows, columns):
        return jax.random.normal(key, (rows, columns), jnp.float32) * rows**-0.5

    drawn = {
        "x": jax.random.normal(jax.random.fold_in(kx, part), (ROWS, D), jnp.float32),
        "gain_a": 1 + 0.1 * jax.random.normal(kn, (D,), jnp.float32),
        "wq": 2 * weights(kq, D, HEADS * HEAD),
        "wk": 2 * weights(kk, D, KV_HEADS * HEAD),
        "wv": 4 * weights(kv, D, KV_HEADS * HEAD),
        "wo": weights(ko, HEADS * HEAD, D),
        "gain_m": 1 + 0.1 * jax.random.normal(km, (D,), jnp.float32),
        "w_gate": weights(kg, D, FF),
        "w_up": weights(ku, D, FF),
        "w_down": 2 * weights(kd, FF, D),
    }
    return {k: v.astype(jnp.bfloat16) for k, v in drawn.items()}


def normed(x, gain):
    wide = x.astype(jnp.float32)
    scale = lax.rsqrt(jnp.mean(wide * wide, -1, keepdims=True) + 1e-6)
    return (wide * scale * gain.astype(jnp.float32)).astype(jnp.bfloat16)


def turned(t, place, theta):
    half = t.shape[-1] // 2
    angle = place.astype(jnp.float32)[:, None] * theta ** (-jnp.arange(half, dtype=jnp.float32) / half)
    cos, sin = jnp.cos(angle)[:, None], jnp.sin(angle)[:, None]
    a, b = t[..., :half].astype(jnp.float32), t[..., half:].astype(jnp.float32)
    return jnp.concatenate([a * cos - b * sin, b * cos + a * sin], -1).astype(jnp.bfloat16)


def matmul(a, w):
    return jnp.dot(a, w, preferred_element_type=jnp.float32).astype(jnp.bfloat16)


def einsum(form, a, b):
    return jnp.einsum(form, a.astype(jnp.float32), b.astype(jnp.float32))


def attention(q, k, v):
    scores = einsum("tgsd,ugd->gstu", q, k) * q.shape[-1] ** -0.5
    token = jnp.arange(q.shape[0])
    scores = jnp.where(token[:, None] >= token, scores, -jnp.inf)
    weights = jax.nn.softmax(scores, -1).astype(jnp.bfloat16)
    return einsum("gstu,ugd->tgsd", weights, v).astype(jnp.bfloat16)


def reference(x, gain_a, wq, wk, wv, wo, gain_m, w_gate, w_up, w_down):
    a, place = normed(x, gain_a), jnp.arange(ROWS)
    q = turned(matmul(a, wq).reshape(ROWS, HEADS, HEAD), place, THETA).reshape(ROWS, KV_HEADS, -1, HEAD)
    k = turned(matmul(a, wk).reshape(ROWS, KV_HEADS, HEAD), place, THETA)
    v = matmul(a, wv).reshape(ROWS, KV_HEADS, HEAD)
    seen = attention(q, k, v).reshape(ROWS, HEADS * HEAD)
    h = (x.astype(jnp.float32) + jnp.dot(seen, wo, preferred_element_type=jnp.float32)).astype(jnp.bfloat16)
    b = normed(h, gain_m)
    gate = jnp.dot(b, w_gate, preferred_element_type=jnp.float32)
    up = jnp.dot(b, w_up, preferred_element_type=jnp.float32)
    hidden = (jax.nn.silu(gate) * up).astype(jnp.bfloat16)
    return (h.astype(jnp.float32) + jnp.dot(hidden, w_down, preferred_element_type=jnp.float32)).astype(jnp.bfloat16)
```

```python
import functools

import jax
import jax.numpy as jnp
from jax import lax
from jax.experimental import pallas as pl
from jax.experimental.pallas import tpu as pltpu
from jax.sharding import PartitionSpec as P

NEG = -1e30
HIDDEN = 2 * NEG
LOG2E = 1.4426950408889634
HEAD = 128
THETA = 10000
SHARES = (64, 96, 96)
FIRST = (208, 48)


def _dot(a, b, ca, cb):
    return lax.dot_general(a, b, (((ca,), (cb,)), ((), ())), preferred_element_type=jnp.float32)


def _turned(t, cos_ref, sin_ref, at):
    t = t.astype(jnp.float32)
    here = pl.ds(pl.multiple_of(at, 16), t.shape[0])
    return (t * cos_ref[here, :] + pltpu.roll(t, HEAD // 2, 1) * sin_ref[here, :]).astype(jnp.bfloat16)


def _keys(kv_ref, cos_ref, sin_ref, k_ref, v_ref):
    block = kv_ref.shape[0]
    k_ref[0] = _turned(kv_ref[:, :HEAD], cos_ref, sin_ref, pl.program_id(0) * block)
    v_ref[0, :HEAD, :] = kv_ref[:, HEAD:].T
    v_ref[0, HEAD:, :] = jnp.ones((8, block), jnp.bfloat16)


def keys(kv, cos, sin, block=512):
    rows = kv.shape[0]
    whole = pl.BlockSpec((rows, HEAD), lambda i: (0, 0))
    return pl.pallas_call(
        _keys,
        grid=(rows // block,),
        in_specs=[pl.BlockSpec((block, 2 * HEAD), lambda i: (i, 0)), whole, whole],
        out_specs=[pl.BlockSpec((1, block, HEAD), lambda i: (i, 0, 0)), pl.BlockSpec((1, HEAD + 8, block), lambda i: (i, 0, 0))],
        out_shape=[jax.ShapeDtypeStruct((rows // block, block, HEAD), jnp.bfloat16), jax.ShapeDtypeStruct((rows // block, HEAD + 8, block), jnp.bfloat16)],
        compiler_params=pltpu.CompilerParams(dimension_semantics=("arbitrary",), vmem_limit_bytes=32 * 2**20),
        cost_estimate=pl.CostEstimate(flops=8 * kv.size, transcendentals=0, bytes_accessed=4 * kv.size),
    )(kv, cos, sin)


def _attention(q_ref, k_ref, v_ref, cos_ref, sin_ref, o_ref, q_s, top_s, mix_s, *, own, start):
    device = pl.program_id(0)
    part, heads = q_ref.shape[1], q_ref.shape[2] // HEAD
    block, cols = k_ref.shape[1], heads * part
    first = device * own + start
    e = HEAD**-0.5 * LOG2E
    for n in range(heads):
        q_s[n * part : (n + 1) * part, :] = _turned(q_ref[0, :, n * HEAD : (n + 1) * HEAD], cos_ref, sin_ref, first)
    top_s[...] = jnp.full(top_s.shape, NEG, jnp.float32)
    mix_s[...] = jnp.zeros(mix_s.shape, jnp.float32)

    def step(j, masked):
        s = _dot(k_ref[j], q_s[...], 1, 1)
        if masked:
            gap = lax.rem(lax.broadcasted_iota(jnp.int32, (block, cols), 1), part) - lax.broadcasted_iota(jnp.int32, (block, cols), 0)
            s = jnp.where(gap >= j * block - first, s, HIDDEN)
        old = top_s[...]
        top = jnp.maximum(old, s.max(axis=0, keepdims=True))
        top_s[...] = top
        p = jnp.exp2((s - top) * e).astype(jnp.bfloat16)
        mix_s[...] = mix_s[...] * jnp.exp2((old - top) * e) + _dot(v_ref[j], p, 1, 0)

    end = first // block
    lax.fori_loop(0, end, lambda j, _: step(j, False), None)
    step(end, True)
    out = (mix_s[:HEAD, :] * (1 / mix_s[HEAD : HEAD + 1, :])).T.astype(o_ref.dtype)
    for n in range(heads):
        o_ref[0, :, n * HEAD : (n + 1) * HEAD] = out[n * part : (n + 1) * part, :]


def attention(q, k, v, cos, sin, own, start):
    devices, part, width = q.shape
    heads = width // HEAD
    cols = heads * part
    whole = lambda t: pl.BlockSpec(t.shape, lambda i: (0,) * t.ndim)
    mine = pl.BlockSpec((1, part, width), lambda i: (i, 0, 0))
    scores = heads * part * devices * k.shape[0] * k.shape[1]
    return pl.pallas_call(
        functools.partial(_attention, own=own, start=start),
        grid=(devices,),
        in_specs=[mine, whole(k), whole(v), whole(cos), whole(sin)],
        out_specs=mine,
        out_shape=jax.ShapeDtypeStruct(q.shape, jnp.bfloat16),
        scratch_shapes=[pltpu.VMEM((cols, HEAD), jnp.bfloat16), pltpu.VMEM((1, cols), jnp.float32), pltpu.VMEM((HEAD + 8, cols), jnp.float32)],
        compiler_params=pltpu.CompilerParams(dimension_semantics=("arbitrary",), vmem_limit_bytes=48 * 2**20),
        cost_estimate=pl.CostEstimate(flops=4 * scores * HEAD, transcendentals=scores, bytes_accessed=4 * q.size),
    )(q, k, v, cos, sin)


def normed(x, gain):
    wide = x.astype(jnp.float32)
    scale = lax.rsqrt(jnp.mean(wide * wide, -1, keepdims=True) + 1e-6)
    return (wide * scale * gain.astype(jnp.float32)).astype(jnp.bfloat16)


def tables(rows):
    half = HEAD // 2
    angle = jnp.arange(rows).astype(jnp.float32)[:, None] * THETA ** (-jnp.arange(half, dtype=jnp.float32) / half)
    cos, sin = jnp.cos(angle), jnp.sin(angle)
    return jnp.concatenate([cos, cos], 1), jnp.concatenate([-sin, sin], 1)


def _gated(*refs):
    *a_refs, gate_ref, up_ref, o_ref = refs
    at = 0
    for a_ref in a_refs:
        dot = lambda w_ref: jnp.dot(a_ref[...], w_ref[...], preferred_element_type=jnp.float32)
        o_ref[at : at + a_ref.shape[0], :] = (jax.nn.silu(dot(gate_ref)) * dot(up_ref)).astype(o_ref.dtype)
        at += a_ref.shape[0]


def gated(parts, w_gate, w_up, half, tile=256):
    rows, depth = sum(p.shape[0] for p in parts), parts[0].shape[1]
    columns = w_gate.shape[1] // 2
    steps = columns // tile
    weights = pl.BlockSpec((depth, tile), lambda j: (0, half * steps + j))
    return pl.pallas_call(
        _gated,
        grid=(steps,),
        in_specs=[pl.BlockSpec(p.shape, lambda j: (0, 0)) for p in parts] + [weights, weights],
        out_specs=pl.BlockSpec((rows, tile), lambda j: (0, j)),
        out_shape=jax.ShapeDtypeStruct((rows, columns), jnp.bfloat16),
        compiler_params=pltpu.CompilerParams(dimension_semantics=("arbitrary",), vmem_limit_bytes=48 * 2**20),
        cost_estimate=pl.CostEstimate(flops=4 * rows * depth * columns, transcendentals=rows * columns, bytes_accessed=4 * depth * columns + 2 * rows * depth),
    )(*parts, w_gate, w_up)


def _term(core_ref, *refs, split):
    *a_refs, w_ref, mine_ref, other_ref, a_s = refs
    chips, part, _ = mine_ref.shape
    half = chips * part
    core = core_ref[0]

    @pl.when(pl.program_id(0) == 0)
    def _():
        at = 0
        for a_ref in a_refs:
            columns = slice(at, at + a_ref.shape[1])
            at += a_ref.shape[1]
            if split:
                a_s[:, columns] = a_ref[...]
                continue
            for chip in range(chips):
                here = slice(chip * part, (chip + 1) * part)
                there = slice(half + chip * part, half + (chip + 1) * part)
                a_s[here, columns] = a_ref[pl.ds(pl.multiple_of((2 * chip + core) * part, 16), part), :]
                a_s[there, columns] = a_ref[pl.ds(pl.multiple_of((2 * chip + 1 - core) * part, 16), part), :]

    t = jnp.dot(a_s[...], w_ref[...], preferred_element_type=jnp.float32)
    mine_ref[...] = t[:half].reshape(mine_ref.shape)
    other_ref[...] = t[half:].reshape(other_ref.shape).astype(other_ref.dtype)


def product(parts, w, core, chips, split, tile=512):
    rows = parts[0].shape[0]
    part = rows // (2 * chips)
    depth, columns = w.shape
    out = pl.BlockSpec((chips, part, tile), lambda j, _: (0, 0, j))
    return pl.pallas_call(
        functools.partial(_term, split=split),
        grid_spec=pltpu.PrefetchScalarGridSpec(
            num_scalar_prefetch=1,
            grid=(columns // tile,),
            in_specs=[pl.BlockSpec(p.shape, lambda j, _: (0, 0)) for p in parts] + [pl.BlockSpec((depth, tile), lambda j, _: (0, j))],
            out_specs=[out, out],
            scratch_shapes=[pltpu.VMEM((rows, depth), jnp.bfloat16)],
        ),
        out_shape=[jax.ShapeDtypeStruct((chips, part, columns), jnp.float32), jax.ShapeDtypeStruct((chips, part, columns), jnp.bfloat16)],
        compiler_params=pltpu.CompilerParams(dimension_semantics=("arbitrary",), vmem_limit_bytes=48 * 2**20),
        cost_estimate=pl.CostEstimate(flops=2 * rows * depth * columns, transcendentals=0, bytes_accessed=2 * depth * columns + 3 * rows * columns),
    )(core, *parts, w)


def tied(*values):
    return lax.optimization_barrier(values)


def later(t, *others):
    return lax.optimization_barrier((t, *others))[0]


def solution(mesh):
    n = mesh.shape["tp"]
    chips = n // 2
    last = chips - 1
    pairs = [(2 * a + c, 2 * b + c) for a in range(chips) for b in (a - 1, a + 1) if 0 <= b < chips for c in range(2)]
    swap = [(i, i ^ 1) for i in range(n)]

    def moves(step, up):
        return [(i, j) for i, j in pairs if (j > i) == up and (i // 2 if up else last - i // 2) <= step]

    def passes(step, up):
        return [(i, j) for i, j in pairs if (j > i) == up and (i // 2 if up else last - i // 2) >= step]

    previous = []

    class Scatter:
        def __init__(self, parts, w, gathered):
            me = lax.axis_index("tp")
            self.chip = me // 2
            self.mine, self.other = product(parts, w, (me % 2)[None].astype(jnp.int32), chips, gathered)
            self.stage, self.gathered = 0, gathered

        def both(self, to):
            to = jnp.clip(to, 0, last)
            if self.gathered:
                to = (self.chip - to + chips) % chips
            pick = lambda t: lax.dynamic_index_in_dim(t, to, 0, keepdims=False).astype(jnp.float32)
            return pick(self.mine) + pick(self.got)

        def sends(self):
            if self.stage == 0:
                return [(self.other, swap)]
            step = self.stage - 1
            up, down = self.both(last - step + self.chip), self.both(step - last + self.chip)
            if step:
                up, down = up + self.ups.astype(jnp.float32), down + self.downs.astype(jnp.float32)
            return [(up.astype(jnp.bfloat16), moves(step, True)), (down.astype(jnp.bfloat16), moves(step, False))]

        def take(self, sent, got):
            if self.stage == 0:
                (self.got,) = got
            else:
                self.ups, self.downs = got
            self.stage += 1

        def sum(self):
            return self.both(self.chip) + self.ups.astype(jnp.float32) + self.downs.astype(jnp.float32)

    class Gather:
        def __init__(self, block):
            self.chip = lax.axis_index("tp") // 2
            self.block, self.ups, self.downs, self.stage = block, [], [], 0

        def sends(self):
            if self.stage < last:
                up, down = (self.ups[-1], self.downs[-1]) if self.stage else (self.block, self.block)
                return [(up, passes(self.stage, True)), (down, passes(self.stage, False))]
            choose = lambda k: jnp.where(self.chip > k, self.ups[k], self.downs[last - 1 - k])
            return [(jnp.concatenate([self.block] + [choose(k) for k in range(last)], 0), swap)]

        def take(self, sent, got):
            if self.stage < last:
                self.ups.append(got[0])
                self.downs.append(got[1])
            else:
                self.parts = [sent[0], got[0]]
            self.stage += 1

    def slot(scatters, work):
        sends = [scatter.sends() for scatter in scatters]
        flat = [s for some in sends for s in some]
        values = tied(*[v for v, _ in flat], *previous)
        got = [lax.ppermute(v, "tp", p) for v, (_, p) in zip(values, flat)]
        done = work([values[0]]) if work else []
        everything = tied(*got, *done)
        previous[:] = everything[-1:]
        at = 0
        for scatter, some in zip(scatters, sends):
            scatter.take(values[at : at + len(some)], everything[at : at + len(some)])
            at += len(some)
        return everything[at:]

    def step(x, gain_a, wq, wk, wv, wo, gain_m, w_gate, w_up, w_down):
        own, width = x.shape
        rows = own * n
        ends = [sum(SHARES[:i]) * own // sum(SHARES) for i in range(len(SHARES) + 1)]
        cut = lambda t, i, axis=0: lax.slice_in_dim(t, ends[i], ends[i + 1], axis=axis)
        fetched = lambda t: lax.all_gather(t, "tp", axis=0, tiled=True)
        plus = lambda t, s: (t.astype(jnp.float32) + s).astype(jnp.bfloat16)
        dot = lambda a, b: jnp.dot(a, b, preferred_element_type=jnp.float32)

        wqkv = jnp.concatenate([wq, wk, wv], 1)
        qkv, at = [], 0
        for share in FIRST:
            count = share * own // sum(FIRST)
            mine = normed(lax.slice_in_dim(x, at, at + count, axis=0), gain_a)
            some = later(fetched(mine), *qkv[-1:])
            qkv.append(dot(some, wqkv).astype(jnp.bfloat16).reshape(n, count, -1))
            at += count
        qkv = jnp.concatenate(qkv, 1)
        split = qkv.shape[2] - 2 * HEAD
        turn = tables(rows)
        k, v = keys(qkv[:, :, split:].reshape(rows, -1), *turn)

        A, B, G, h, b, hidden, seen = {}, {}, {}, {}, {}, {}, {}
        out = {}

        def attend(i):
            def work(hold):
                seen[i] = attention(hold(cut(qkv[:, :, :split], i, 1)), k, v, *turn, own, ends[i])
                return [seen[i]]

            def keep(values):
                (seen[i],) = values

            return work, keep

        def out_proj(i):
            def work(hold):
                A[i] = Scatter([hold(seen[i].reshape(-1, split))], wo, False)
                return [A[i].mine, A[i].other]

            def keep(values):
                A[i].mine, A[i].other = values

            return work, keep

        def norm(i):
            def work(hold):
                h[i] = plus(hold(cut(x, i)), A[i].sum())
                b[i] = normed(h[i], gain_m)
                return [h[i], b[i]]

            def keep(values):
                h[i], b[i] = values
                G[i] = Gather(b[i])

            return work, keep

        def inner(i, half):
            def work(hold):
                hidden[i, half] = gated([hold(G[i].parts[0]), G[i].parts[1]], w_gate, w_up, half)
                return [hidden[i, half]]

            def keep(values):
                (hidden[i, half],) = values

            return work, keep

        def downed(i):
            def work(hold):
                B[i] = Scatter([hold(hidden[i, 0]), hidden[i, 1]], w_down, True)
                return [B[i].mine, B[i].other]

            def keep(values):
                B[i].mine, B[i].other = values

            return work, keep

        def finish(i):
            def work(hold):
                out[i] = plus(hold(h[i]), B[i].sum())
                return [out[i]]

            def keep(values):
                (out[i],) = values

            return work, keep

        def run(scatters, *works):
            counts = []

            def work(after):
                done = []
                for w, _ in works:
                    some = w(lambda t: later(t, *after))
                    after = some[-1:]
                    counts.append(len(some))
                    done += some
                return done

            done = slot([s[i] for s, i in scatters], work if works else None)
            at = 0
            for (_, keep), count in zip(works, counts):
                keep(done[at : at + count])
                at += count

        previous.clear()
        for first, _ in (attend(0), out_proj(0)):
            first(lambda t: t)
        run([(A, 0)])
        run([(A, 0)], attend(1))
        run([(A, 0)], out_proj(1))
        run([(A, 0), (A, 1)], attend(2))
        run([], norm(0))
        run([(G, 0)], out_proj(2))
        run([(A, 1), (G, 0)])
        run([(A, 1), (A, 2), (G, 0)])
        run([(A, 1), (G, 0)])
        run([], norm(1))
        run([(G, 1)], inner(0, 0))
        run([(A, 2), (G, 1)], inner(0, 1))
        run([(A, 2), (G, 1)], downed(0))
        run([(A, 2), (G, 1), (B, 0)])
        run([], norm(2))
        run([(G, 2)], inner(1, 0))
        run([(B, 0), (G, 2)], inner(1, 1))
        run([(B, 0), (G, 2)], downed(1))
        run([(B, 0), (G, 2), (B, 1)])
        run([(B, 1)], inner(2, 0))
        run([(B, 1)], inner(2, 1))
        run([(B, 1)], finish(0), downed(2))
        run([(B, 2)])
        run([(B, 2)], finish(1))
        run([(B, 2)])
        run([(B, 2)])
        last_one, _ = finish(2)
        last_one(lambda t: t)
        return jnp.concatenate([out[i] for i in range(len(SHARES))], 0)

    tokens, columns, rows_of = P(("dp", "tp"), None), P(None, "tp"), P("tp", None)
    return jax.shard_map(
        step,
        mesh=mesh,
        in_specs=(tokens, P(None), columns, columns, columns, rows_of, P(None), columns, columns, rows_of),
        out_specs=tokens,
        check_vma=False,
    )
```

```python
import functools

import jax
import jax.numpy as jnp
from jax import lax
from jax.experimental import pallas as pl
from jax.experimental.pallas import tpu as pltpu
from jax.sharding import PartitionSpec as P


NEG = -1e30
HIDDEN = 2 * NEG
LOG2E = 1.4426950408889634
HEAD = 128
THETA = 10000
SHARES = (64, 96, 96)
FIRST = (208, 48)


def _dot(a, b, ca, cb):
    return lax.dot_general(a, b, (((ca,), (cb,)), ((), ())), preferred_element_type=jnp.float32)


def _turned(t, cos_ref, sin_ref, at):
    t = t.astype(jnp.float32)
    here = pl.ds(pl.multiple_of(at, 16), t.shape[0])
    return (t * cos_ref[here, :] + pltpu.roll(t, HEAD // 2, 1) * sin_ref[here, :]).astype(jnp.bfloat16)


def _keys(kv_ref, cos_ref, sin_ref, k_ref, v_ref):
    block = kv_ref.shape[0]
    k_ref[0] = _turned(kv_ref[:, :HEAD], cos_ref, sin_ref, pl.program_id(0) * block)
    v_ref[0, :HEAD, :] = kv_ref[:, HEAD:].T
    v_ref[0, HEAD:, :] = jnp.ones((8, block), jnp.bfloat16)


def keys(kv, cos, sin, block=512):
    rows = kv.shape[0]
    whole = pl.BlockSpec((rows, HEAD), lambda i: (0, 0))
    return pl.pallas_call(
        _keys,
        grid=(rows // block,),
        in_specs=[pl.BlockSpec((block, 2 * HEAD), lambda i: (i, 0)), whole, whole],
        out_specs=[pl.BlockSpec((1, block, HEAD), lambda i: (i, 0, 0)), pl.BlockSpec((1, HEAD + 8, block), lambda i: (i, 0, 0))],
        out_shape=[jax.ShapeDtypeStruct((rows // block, block, HEAD), jnp.bfloat16), jax.ShapeDtypeStruct((rows // block, HEAD + 8, block), jnp.bfloat16)],
        compiler_params=pltpu.CompilerParams(dimension_semantics=("arbitrary",), vmem_limit_bytes=32 * 2**20),
        cost_estimate=pl.CostEstimate(flops=8 * kv.size, transcendentals=0, bytes_accessed=4 * kv.size),
    )(kv, cos, sin)


def _attention(q_ref, k_ref, v_ref, cos_ref, sin_ref, o_ref, q_s, top_s, mix_s, *, own, start):
    device = pl.program_id(0)
    part, heads = q_ref.shape[1], q_ref.shape[2] // HEAD
    block, cols = k_ref.shape[1], heads * part
    first = device * own + start
    e = HEAD**-0.5 * LOG2E
    for n in range(heads):
        q_s[n * part : (n + 1) * part, :] = _turned(q_ref[0, :, n * HEAD : (n + 1) * HEAD], cos_ref, sin_ref, first)
    top_s[...] = jnp.full(top_s.shape, NEG, jnp.float32)
    mix_s[...] = jnp.zeros(mix_s.shape, jnp.float32)

    def step(j, masked):
        s = _dot(k_ref[j], q_s[...], 1, 1)
        if masked:
            gap = lax.rem(lax.broadcasted_iota(jnp.int32, (block, cols), 1), part) - lax.broadcasted_iota(jnp.int32, (block, cols), 0)
            s = jnp.where(gap >= j * block - first, s, HIDDEN)
        old = top_s[...]
        top = jnp.maximum(old, s.max(axis=0, keepdims=True))
        top_s[...] = top
        p = jnp.exp2((s - top) * e).astype(jnp.bfloat16)
        mix_s[...] = mix_s[...] * jnp.exp2((old - top) * e) + _dot(v_ref[j], p, 1, 0)

    end = first // block
    lax.fori_loop(0, end, lambda j, _: step(j, False), None)
    step(end, True)
    out = (mix_s[:HEAD, :] * (1 / mix_s[HEAD : HEAD + 1, :])).T.astype(o_ref.dtype)
    for n in range(heads):
        o_ref[0, :, n * HEAD : (n + 1) * HEAD] = out[n * part : (n + 1) * part, :]


def attention(q, k, v, cos, sin, own, start):
    devices, part, width = q.shape
    heads = width // HEAD
    cols = heads * part
    whole = lambda t: pl.BlockSpec(t.shape, lambda i: (0,) * t.ndim)
    mine = pl.BlockSpec((1, part, width), lambda i: (i, 0, 0))
    scores = heads * part * devices * k.shape[0] * k.shape[1]
    return pl.pallas_call(
        functools.partial(_attention, own=own, start=start),
        grid=(devices,),
        in_specs=[mine, whole(k), whole(v), whole(cos), whole(sin)],
        out_specs=mine,
        out_shape=jax.ShapeDtypeStruct(q.shape, jnp.bfloat16),
        scratch_shapes=[pltpu.VMEM((cols, HEAD), jnp.bfloat16), pltpu.VMEM((1, cols), jnp.float32), pltpu.VMEM((HEAD + 8, cols), jnp.float32)],
        compiler_params=pltpu.CompilerParams(dimension_semantics=("arbitrary",), vmem_limit_bytes=48 * 2**20),
        cost_estimate=pl.CostEstimate(flops=4 * scores * HEAD, transcendentals=scores, bytes_accessed=4 * q.size),
    )(q, k, v, cos, sin)


def normed(x, gain):
    wide = x.astype(jnp.float32)
    scale = lax.rsqrt(jnp.mean(wide * wide, -1, keepdims=True) + 1e-6)
    return (wide * scale * gain.astype(jnp.float32)).astype(jnp.bfloat16)


def tables(rows):
    half = HEAD // 2
    angle = jnp.arange(rows).astype(jnp.float32)[:, None] * THETA ** (-jnp.arange(half, dtype=jnp.float32) / half)
    cos, sin = jnp.cos(angle), jnp.sin(angle)
    return jnp.concatenate([cos, cos], 1), jnp.concatenate([-sin, sin], 1)


def _gated(*refs):
    *a_refs, gate_ref, up_ref, o_ref = refs
    at = 0
    for a_ref in a_refs:
        dot = lambda w_ref: jnp.dot(a_ref[...], w_ref[...], preferred_element_type=jnp.float32)
        o_ref[at : at + a_ref.shape[0], :] = (jax.nn.silu(dot(gate_ref)) * dot(up_ref)).astype(o_ref.dtype)
        at += a_ref.shape[0]


def gated(parts, w_gate, w_up, half, tile=256):
    rows, depth = sum(p.shape[0] for p in parts), parts[0].shape[1]
    columns = w_gate.shape[1] // 2
    steps = columns // tile
    weights = pl.BlockSpec((depth, tile), lambda j: (0, half * steps + j))
    return pl.pallas_call(
        _gated,
        grid=(steps,),
        in_specs=[pl.BlockSpec(p.shape, lambda j: (0, 0)) for p in parts] + [weights, weights],
        out_specs=pl.BlockSpec((rows, tile), lambda j: (0, j)),
        out_shape=jax.ShapeDtypeStruct((rows, columns), jnp.bfloat16),
        compiler_params=pltpu.CompilerParams(dimension_semantics=("arbitrary",), vmem_limit_bytes=48 * 2**20),
        cost_estimate=pl.CostEstimate(flops=4 * rows * depth * columns, transcendentals=rows * columns, bytes_accessed=4 * depth * columns + 2 * rows * depth),
    )(*parts, w_gate, w_up)


def _term(core_ref, *refs, split):
    *a_refs, w_ref, mine_ref, other_ref, a_s = refs
    chips, part, _ = mine_ref.shape
    half = chips * part
    core = core_ref[0]

    @pl.when(pl.program_id(0) == 0)
    def _():
        at = 0
        for a_ref in a_refs:
            columns = slice(at, at + a_ref.shape[1])
            at += a_ref.shape[1]
            if split:
                a_s[:, columns] = a_ref[...]
                continue
            for chip in range(chips):
                here = slice(chip * part, (chip + 1) * part)
                there = slice(half + chip * part, half + (chip + 1) * part)
                a_s[here, columns] = a_ref[pl.ds(pl.multiple_of((2 * chip + core) * part, 16), part), :]
                a_s[there, columns] = a_ref[pl.ds(pl.multiple_of((2 * chip + 1 - core) * part, 16), part), :]

    t = jnp.dot(a_s[...], w_ref[...], preferred_element_type=jnp.float32)
    mine_ref[...] = t[:half].reshape(mine_ref.shape)
    other_ref[...] = t[half:].reshape(other_ref.shape).astype(other_ref.dtype)


def product(parts, w, core, chips, split, tile=512):
    rows = parts[0].shape[0]
    part = rows // (2 * chips)
    depth, columns = w.shape
    out = pl.BlockSpec((chips, part, tile), lambda j, _: (0, 0, j))
    return pl.pallas_call(
        functools.partial(_term, split=split),
        grid_spec=pltpu.PrefetchScalarGridSpec(
            num_scalar_prefetch=1,
            grid=(columns // tile,),
            in_specs=[pl.BlockSpec(p.shape, lambda j, _: (0, 0)) for p in parts] + [pl.BlockSpec((depth, tile), lambda j, _: (0, j))],
            out_specs=[out, out],
            scratch_shapes=[pltpu.VMEM((rows, depth), jnp.bfloat16)],
        ),
        out_shape=[jax.ShapeDtypeStruct((chips, part, columns), jnp.float32), jax.ShapeDtypeStruct((chips, part, columns), jnp.bfloat16)],
        compiler_params=pltpu.CompilerParams(dimension_semantics=("arbitrary",), vmem_limit_bytes=48 * 2**20),
        cost_estimate=pl.CostEstimate(flops=2 * rows * depth * columns, transcendentals=0, bytes_accessed=2 * depth * columns + 3 * rows * columns),
    )(core, *parts, w)


def tied(*values):
    return lax.optimization_barrier(values)


def later(t, *others):
    return lax.optimization_barrier((t, *others))[0]


def solution(mesh):
    n = mesh.shape["tp"]
    chips = n // 2
    last = chips - 1
    pairs = [(2 * a + c, 2 * b + c) for a in range(chips) for b in (a - 1, a + 1) if 0 <= b < chips for c in range(2)]
    swap = [(i, i ^ 1) for i in range(n)]

    def moves(step, up):
        return [(i, j) for i, j in pairs if (j > i) == up and (i // 2 if up else last - i // 2) <= step]

    def passes(step, up):
        return [(i, j) for i, j in pairs if (j > i) == up and (i // 2 if up else last - i // 2) >= step]

    previous = []

    class Scatter:
        def __init__(self, parts, w, gathered):
            me = lax.axis_index("tp")
            self.chip = me // 2
            self.mine, self.other = product(parts, w, (me % 2)[None].astype(jnp.int32), chips, gathered)
            self.stage, self.gathered = 0, gathered

        def both(self, to):
            to = jnp.clip(to, 0, last)
            if self.gathered:
                to = (self.chip - to + chips) % chips
            pick = lambda t: lax.dynamic_index_in_dim(t, to, 0, keepdims=False).astype(jnp.float32)
            return pick(self.mine) + pick(self.got)

        def sends(self):
            if self.stage == 0:
                return [(self.other, swap)]
            step = self.stage - 1
            up, down = self.both(last - step + self.chip), self.both(step - last + self.chip)
            if step:
                up, down = up + self.ups.astype(jnp.float32), down + self.downs.astype(jnp.float32)
            return [(up.astype(jnp.bfloat16), moves(step, True)), (down.astype(jnp.bfloat16), moves(step, False))]

        def take(self, sent, got):
            if self.stage == 0:
                (self.got,) = got
            else:
                self.ups, self.downs = got
            self.stage += 1

        def sum(self):
            return self.both(self.chip) + self.ups.astype(jnp.float32) + self.downs.astype(jnp.float32)

    class Gather:
        def __init__(self, block):
            self.chip = lax.axis_index("tp") // 2
            self.block, self.ups, self.downs, self.stage = block, [], [], 0

        def sends(self):
            if self.stage < last:
                up, down = (self.ups[-1], self.downs[-1]) if self.stage else (self.block, self.block)
                return [(up, passes(self.stage, True)), (down, passes(self.stage, False))]
            choose = lambda k: jnp.where(self.chip > k, self.ups[k], self.downs[last - 1 - k])
            return [(jnp.concatenate([self.block] + [choose(k) for k in range(last)], 0), swap)]

        def take(self, sent, got):
            if self.stage < last:
                self.ups.append(got[0])
                self.downs.append(got[1])
            else:
                self.parts = [sent[0], got[0]]
            self.stage += 1

    def slot(scatters, work):
        sends = [scatter.sends() for scatter in scatters]
        flat = [s for some in sends for s in some]
        values = tied(*[v for v, _ in flat], *previous)
        got = []
        for v, (_, p) in zip(values, flat):
            got.append(lax.ppermute(v, "tp", p))
        done = work([values[0]]) if work else []
        everything = tied(*got, *done)
        previous[:] = everything[-1:]
        at = 0
        for scatter, some in zip(scatters, sends):
            scatter.take(values[at : at + len(some)], everything[at : at + len(some)])
            at += len(some)
        return everything[at:]

    def layer(x, gain_a, wq, wk, wv, wo, gain_m, w_gate, w_up, w_down):
        own, _ = x.shape
        rows = own * n
        ends = [sum(SHARES[:i]) * own // sum(SHARES) for i in range(len(SHARES) + 1)]
        cut = lambda t, i, axis=0: lax.slice_in_dim(t, ends[i], ends[i + 1], axis=axis)
        fetched = lambda t: lax.all_gather(t, "tp", axis=0, tiled=True)
        plus = lambda t, s: (t.astype(jnp.float32) + s).astype(jnp.bfloat16)
        dot = lambda a, b: jnp.dot(a, b, preferred_element_type=jnp.float32)

        wqkv = jnp.concatenate([wq, wk, wv], 1)
        qkv, at = [], 0
        for share in FIRST:
            count = share * own // sum(FIRST)
            mine = normed(lax.slice_in_dim(x, at, at + count, axis=0), gain_a)
            some = later(fetched(mine), *qkv[-1:])
            qkv.append(dot(some, wqkv).astype(jnp.bfloat16).reshape(n, count, -1))
            at += count
        qkv = jnp.concatenate(qkv, 1)
        split = qkv.shape[2] - 2 * HEAD
        turn = tables(rows)
        k, v = keys(qkv[:, :, split:].reshape(rows, -1), *turn)

        A, B, G, h, b, hidden, seen = {}, {}, {}, {}, {}, {}, {}
        out = {}

        def attend(i):
            def work(hold):
                seen[i] = attention(hold(cut(qkv[:, :, :split], i, 1)), k, v, *turn, own, ends[i])
                return [seen[i]]

            def keep(values):
                (seen[i],) = values

            return work, keep

        def out_proj(i):
            def work(hold):
                A[i] = Scatter([hold(seen[i].reshape(-1, split))], wo, False)
                return [A[i].mine, A[i].other]

            def keep(values):
                A[i].mine, A[i].other = values

            return work, keep

        def norm(i):
            def work(hold):
                h[i] = plus(hold(cut(x, i)), A[i].sum())
                b[i] = normed(h[i], gain_m)
                return [h[i], b[i]]

            def keep(values):
                h[i], b[i] = values
                G[i] = Gather(b[i])

            return work, keep

        def inner(i, half):
            def work(hold):
                hidden[i, half] = gated([hold(G[i].parts[0]), G[i].parts[1]], w_gate, w_up, half)
                return [hidden[i, half]]

            def keep(values):
                (hidden[i, half],) = values

            return work, keep

        def downed(i):
            def work(hold):
                B[i] = Scatter([hold(hidden[i, 0]), hidden[i, 1]], w_down, True)
                return [B[i].mine, B[i].other]

            def keep(values):
                B[i].mine, B[i].other = values

            return work, keep

        def finish(i):
            def work(hold):
                out[i] = plus(hold(h[i]), B[i].sum())
                return [out[i]]

            def keep(values):
                (out[i],) = values

            return work, keep

        def run(scatters, *works):
            counts = []

            def work(after):
                done = []
                for w, _ in works:
                    some = w(lambda t: later(t, *after))
                    after = some[-1:]
                    counts.append(len(some))
                    done += some
                return done

            done = slot([s[i] for s, i in scatters], work if works else None)
            at = 0
            for (_, keep), count in zip(works, counts):
                keep(done[at : at + count])
                at += count

        previous.clear()
        for first, _ in (attend(0), out_proj(0)):
            first(lambda t: t)
        run([(A, 0)])
        run([(A, 0)], attend(1))
        run([(A, 0)], out_proj(1))
        run([(A, 0), (A, 1)], attend(2))
        run([], norm(0))
        run([(G, 0)], out_proj(2))
        run([(A, 1), (G, 0)])
        run([(A, 1), (A, 2), (G, 0)])
        run([(A, 1), (G, 0)])
        run([], norm(1))
        run([(G, 1)], inner(0, 0))
        run([(A, 2), (G, 1)], inner(0, 1))
        run([(A, 2), (G, 1)], downed(0))
        run([(A, 2), (G, 1), (B, 0)])
        run([], norm(2))
        run([(G, 2)], inner(1, 0))
        run([(B, 0), (G, 2)], inner(1, 1))
        run([(B, 0), (G, 2)], downed(1))
        run([(B, 0), (G, 2), (B, 1)])
        run([(B, 1)], inner(2, 0))
        run([(B, 1)], inner(2, 1))
        run([(B, 1)], finish(0), downed(2))
        run([(B, 2)])
        run([(B, 2)], finish(1))
        run([(B, 2)])
        run([(B, 2)])
        last_one, _ = finish(2)
        last_one(lambda t: t)
        return jnp.concatenate([out[i] for i in range(len(SHARES))], 0)

    tokens, columns, rows_of = P(("dp", "tp"), None), P(None, "tp"), P("tp", None)
    return jax.shard_map(
        layer,
        mesh=mesh,
        in_specs=(tokens, P(None), columns, columns, columns, rows_of, P(None), columns, columns, rows_of),
        out_specs=tokens,
        check_vma=False,
    )
```
